512 devices in a mesh: slab: 64 (over z, x, core), tile: 8 (over y).
Axes of the slice: x: 4, y: 8, z: 8, core: 2. Of those that a mesh axis runs over, the one named last changes fastest.
Arguments:
- features: bfloat16 [64, 8, 512, 128], P('slab', 'tile'), may hold values from -24 to 24
- counts: int32 [64, 8], P('slab', 'tile'), may hold values from 128 to 512, as said below
- rulebook: int32 [64, 8, 27, 512], P('slab', 'tile'), may hold values from 0 to 800, as said below
- face_rows: int32 [64, 8, 4, 64], P('slab', 'tile'), may hold values from 0 to 511, as said below
- conv_one: bfloat16 [27, 128, 128], replicated, may hold values from -0.109375 to 0.109375
- gain_one: float32 [128], replicated, may hold values from 0.5 to 1.5
- shift_one: float32 [128], replicated, may hold values from -0.5 to 0.5
- conv_two: bfloat16 [27, 128, 128], replicated, may hold values from -0.109375 to 0.109375
- gain_two: float32 [128], replicated, may hold values from 0.5 to 1.5
- shift_two: float32 [128], replicated, may hold values from -0.5 to 0.5
Outputs:
- output: bfloat16 [64, 8, 512, 128], P('slab', 'tile')
The draws below stay inside these ranges and needn't reach their ends.
Inputs may be any that keep to these rules, and one draw needn't show every extreme that they name: `counts`: each device's voxels fill its 8 x 8 grid columns with the same number each, between 2 and 8; some device of the highest slab index holds 512. `rulebook`: an entry names the extended-table row that holds the voxel's neighbour at offset k = 9 (dx + 1) + 3 (dy + 1) + (dz + 1) of the submanifold 3x3x3 stencil, or 800 where that cell is inactive or outside the grid; the voxel itself is at offset 13; rows at or past the device's count name 800 at every offset. `face_rows`: lists 0 to 3 hold the device's voxels on its lower and higher face along the first, then the lower and higher face along the second dimension; the j-th voxel of the i-th column along a face stands at position i * 8 + j; unused positions name row 0.
All inputs are finite; a program needn't handle non-finite values.
Results may differ from the reference program's by a relative error of at most 0.0033.
Values may be sent and summed in bfloat16 or wider, within the bound.
A program may use at most 64 MiB of HBM per device.

```python
import math
import jax
import jax.numpy as jnp
from jax import lax

CHANNELS = 128
SIDE = 8
COLUMN = 8
DEPTH = 512
ROWS = 512
FACE = 64
TABLE = 800
N_SLAB = 64
N_TILE = 8


def voxel_layout(key):
    base_key = jax.random.fold_in(key, 11)
    coin_key, pick_key, depth_key = jax.random.split(base_key, 3)
    quarter = COLUMN // 4
    slab_ramp = quarter + (COLUMN - quarter) * jnp.arange(N_SLAB, dtype=jnp.int32) // max(N_SLAB - 1, 1)
    coin_flip = jax.random.randint(coin_key, (N_SLAB, N_TILE), 0, 2)
    per_column = jnp.where(coin_flip == 0, slab_ramp[:, None], quarter).astype(jnp.int32)
    chosen = jax.random.randint(pick_key, (), 0, N_TILE)
    per_column = per_column.at[N_SLAB - 1, chosen].set(COLUMN)
    column_total = N_SLAB * N_TILE * SIDE * SIDE
    depth_keys = jax.random.split(depth_key, column_total)
    shuffled = jax.vmap(lambda one_key: jax.random.permutation(one_key, DEPTH)[:COLUMN])(depth_keys)
    shuffled = shuffled.astype(jnp.int32).reshape(N_SLAB, N_TILE, SIDE, SIDE, COLUMN)
    rank_list = jnp.arange(COLUMN, dtype=jnp.int32)
    full_shape = (N_SLAB, N_TILE, SIDE, SIDE, COLUMN)
    own_count = jnp.broadcast_to(per_column[:, :, None, None, None], full_shape)
    filled = jnp.broadcast_to(rank_list, full_shape) < own_count
    depth_pos = jnp.sort(jnp.where(filled, shuffled, DEPTH + COLUMN), axis=-1)
    local_slab = jnp.broadcast_to(jnp.arange(SIDE, dtype=jnp.int32)[None, None, :, None, None], full_shape)
    local_tile = jnp.broadcast_to(jnp.arange(SIDE, dtype=jnp.int32)[None, None, None, :, None], full_shape)
    slab_index = jnp.broadcast_to(jnp.arange(N_SLAB, dtype=jnp.int32)[:, None, None, None, None], full_shape)
    tile_index = jnp.broadcast_to(jnp.arange(N_TILE, dtype=jnp.int32)[None, :, None, None, None], full_shape)
    slab_cell = slab_index * SIDE + local_slab
    tile_cell = tile_index * SIDE + local_tile
    rank_full = jnp.broadcast_to(rank_list, full_shape)
    occupancy = jnp.full((N_SLAB * SIDE, N_TILE * SIDE, DEPTH), -1, jnp.int32)
    occupancy = occupancy.at[slab_cell, tile_cell, depth_pos].set(rank_full, mode='drop')
    tap_values = []
    for shift_slab in range(-1, 2):
        for shift_tile in range(-1, 2):
            for shift_depth in range(-1, 2):
                near_slab = local_slab + shift_slab
                near_tile = local_tile + shift_tile
                near_depth = depth_pos + shift_depth
                cell_slab = slab_cell + shift_slab
                cell_tile = tile_cell + shift_tile
                inside = (cell_slab >= 0) & (cell_slab < N_SLAB * SIDE) & (cell_tile >= 0) & (cell_tile < N_TILE * SIDE)
                inside = inside & (near_depth >= 0) & (near_depth < DEPTH) & filled
                found_rank = occupancy[jnp.clip(cell_slab, 0, N_SLAB * SIDE - 1), jnp.clip(cell_tile, 0, N_TILE * SIDE - 1), jnp.clip(near_depth, 0, DEPTH - 1)]
                present = inside & (found_rank >= 0)
                in_slab = (near_slab >= 0) & (near_slab < SIDE)
                in_tile = (near_tile >= 0) & (near_tile < SIDE)
                own_index = (near_slab * SIDE + near_tile) * own_count + found_rank
                slab_index_low = ROWS + near_tile * COLUMN + found_rank
                slab_index_high = ROWS + FACE + near_tile * COLUMN + found_rank
                tile_index_low = ROWS + 2 * FACE + (near_slab + 1) * COLUMN + found_rank
                tile_index_high = ROWS + 3 * FACE + 2 * COLUMN + (near_slab + 1) * COLUMN + found_rank
                local_index = jnp.where(in_slab & in_tile, own_index, jnp.where(in_tile, jnp.where(near_slab < 0, slab_index_low, slab_index_high), jnp.where(near_tile < 0, tile_index_low, tile_index_high)))
                tap_values.append(jnp.where(present, local_index, TABLE).astype(jnp.int32))
    stacked = jnp.stack(tap_values, axis=2)
    big_shape = (N_SLAB, N_TILE, 27, SIDE, SIDE, COLUMN)
    row_target = jnp.where(filled, (local_slab * SIDE + local_tile) * own_count + rank_full, ROWS)
    row_target = jnp.broadcast_to(row_target[:, :, None], big_shape)
    slab_target = jnp.broadcast_to(slab_index[:, :, None], big_shape)
    tile_target = jnp.broadcast_to(tile_index[:, :, None], big_shape)
    tap_target = jnp.broadcast_to(jnp.arange(27, dtype=jnp.int32)[None, None, :, None, None, None], big_shape)
    rulebook = jnp.full((N_SLAB, N_TILE, 27, ROWS), TABLE, jnp.int32)
    rulebook = rulebook.at[slab_target, tile_target, tap_target, row_target].set(stacked, mode='drop')
    along_face = jnp.arange(SIDE, dtype=jnp.int32)[None, None, :, None]
    face_rank = rank_list[None, None, None, :]
    face_count = per_column[:, :, None, None]
    face_filled = face_rank < face_count
    slab_lower = (0 * SIDE + along_face) * face_count + face_rank
    slab_upper = ((SIDE - 1) * SIDE + along_face) * face_count + face_rank
    tile_lower = (along_face * SIDE + 0) * face_count + face_rank
    tile_upper = (along_face * SIDE + SIDE - 1) * face_count + face_rank
    face_lists = []
    for face_list in (slab_lower, slab_upper, tile_lower, tile_upper):
        face_lists.append(jnp.where(face_filled, face_list, 0).reshape(N_SLAB, N_TILE, FACE))
    face_rows = jnp.stack(face_lists, axis=2).astype(jnp.int32)
    counts = (per_column * SIDE * SIDE).astype(jnp.int32)
    return (counts, rulebook, face_rows)


def draw_counts(key, part):
    return voxel_layout(key)[0]


def draw_rulebook(key, part):
    return voxel_layout(key)[1]


def draw_face_rows(key, part):
    return voxel_layout(key)[2]


def draw_features(key, part):
    noise_key, row_key, chan_key = jax.random.split(jax.random.fold_in(key, 23), 3)
    array_shape = (N_SLAB, N_TILE, ROWS, CHANNELS)
    row_scale = jnp.exp(jax.random.uniform(row_key, (N_SLAB, N_TILE, ROWS, 1), jnp.float32, math.log(0.3), math.log(3.0)))
    chan_scale = jnp.exp(jax.random.uniform(chan_key, (CHANNELS,), jnp.float32, math.log(0.5), math.log(2.0)))
    base_noise = jnp.clip(jax.random.normal(noise_key, array_shape, jnp.float32), -4.0, 4.0)
    return (base_noise * row_scale * chan_scale).astype(jnp.bfloat16)


def gaussian(own_key, extent, spread, limit, held_as=jnp.bfloat16):
    return jnp.clip(spread * jax.random.normal(own_key, extent, jnp.float32), -limit, limit).astype(held_as)


def setup_inputs(seed: int = 0) -> dict:
    streams_of = jax.random.split(jax.random.key(seed), 11)
    return {
        "features": draw_features(jax.random.fold_in(streams_of[10], 71), 0),
        "counts": draw_counts(jax.random.fold_in(streams_of[10], 71), 0),
        "rulebook": draw_rulebook(jax.random.fold_in(streams_of[10], 71), 0),
        "face_rows": draw_face_rows(jax.random.fold_in(streams_of[10], 71), 0),
        "conv_one": gaussian(streams_of[4], (27, CHANNELS, CHANNELS), (27 * CHANNELS) ** -0.5, 0.109375),
        "gain_one": jnp.clip(1.0 + 0.1 * jax.random.normal(streams_of[5], (CHANNELS,), jnp.float32), 0.5, 1.5),
        "shift_one": jnp.clip(jax.random.uniform(streams_of[6], (CHANNELS,), jnp.float32, -0.5, 0.5), -0.5, 0.5),
        "conv_two": gaussian(streams_of[7], (27, CHANNELS, CHANNELS), (27 * CHANNELS) ** -0.5, 0.109375),
        "gain_two": jnp.clip(1.0 + 0.1 * jax.random.normal(streams_of[8], (CHANNELS,), jnp.float32), 0.5, 1.5),
        "shift_two": jnp.clip(jax.random.uniform(streams_of[9], (CHANNELS,), jnp.float32, -0.5, 0.5), -0.5, 0.5),
    }


EPSILON = 1e-05

def extend(voxel_rows, face_rows):
    picked = jax.vmap(jax.vmap(lambda row_list, positions: row_list[positions]))(voxel_rows, face_rows)
    blank = jnp.zeros_like(picked[:1, :, 0])
    slab_low = jnp.concatenate([blank, picked[:-1, :, 1]], axis=0)
    slab_high = jnp.concatenate([picked[1:, :, 0], blank], axis=0)
    lower_send = jnp.concatenate([slab_low[:, :, :COLUMN], picked[:, :, 2], slab_high[:, :, :COLUMN]], axis=2)
    upper_send = jnp.concatenate([slab_low[:, :, FACE - COLUMN:], picked[:, :, 3], slab_high[:, :, FACE - COLUMN:]], axis=2)
    edge_rows = jnp.zeros_like(lower_send[:, :1])
    tile_low = jnp.concatenate([edge_rows, upper_send[:, :-1]], axis=1)
    tile_high = jnp.concatenate([lower_send[:, 1:], edge_rows], axis=1)
    zero_row = jnp.zeros_like(voxel_rows[:, :, :1])
    return jnp.concatenate([voxel_rows, slab_low, slab_high, tile_low, tile_high, zero_row], axis=2)

def convolve_all(lookup, rulebook, weight):
    device_count = N_SLAB * N_TILE
    flat_weight = weight.astype(jnp.float32).reshape(27 * CHANNELS, CHANNELS)
    tables = lookup.reshape(device_count, TABLE + 1, CHANNELS)
    indices = rulebook.reshape(device_count, 27, ROWS)

    def one_device(pair):
        table_rows, tap_rows = pair
        gathered = table_rows[tap_rows.T].reshape(ROWS, 27 * CHANNELS).astype(jnp.float32)
        return jnp.dot(gathered, flat_weight, preferred_element_type=jnp.float32)
    result = lax.map(one_device, (tables, indices))
    return result.reshape(N_SLAB, N_TILE, ROWS, CHANNELS)

def normalize(conv_out, live_mask, voxel_total, gain, shift):
    average = lax.optimization_barrier(jnp.sum(conv_out * live_mask, axis=(0, 1, 2))) / voxel_total
    centred = (conv_out - average) * live_mask
    variance = lax.optimization_barrier(jnp.sum(centred * centred, axis=(0, 1, 2))) / voxel_total
    return (conv_out - average) / jnp.sqrt(variance + EPSILON) * gain + shift

def reference(features, counts, rulebook, face_rows, conv_one, gain_one, shift_one, conv_two, gain_two, shift_two):
    live_mask = (jnp.arange(ROWS, dtype=jnp.int32)[None, None, :] < counts[:, :, None]).astype(jnp.float32)[..., None]
    voxel_total = jnp.sum(counts).astype(jnp.float32)
    first = convolve_all(extend(features, face_rows), rulebook, conv_one)
    hidden = (live_mask * jnp.maximum(normalize(first, live_mask, voxel_total, gain_one, shift_one), 0.0)).astype(jnp.bfloat16)
    second = convolve_all(extend(hidden, face_rows), rulebook, conv_two)
    summed = normalize(second, live_mask, voxel_total, gain_two, shift_two) + features.astype(jnp.float32)
    return (live_mask * jnp.maximum(summed, 0.0)).astype(jnp.bfloat16)
```

```python
import functools

import jax
import jax.numpy as jnp
from jax import lax
from jax.experimental import pallas as pl
from jax.experimental.pallas import tpu as pltpu
from jax.sharding import PartitionSpec as P

MESH = pl.DeviceIdType.MESH
F32 = jnp.float32
BF16 = jnp.bfloat16
EPSILON = 1e-05
DEAD = -1e30
RING = 8
TAPS = 27
HALF = 256
HALO = 288


def thirds(x):
    high = x.astype(BF16)
    rest = x - high.astype(F32)
    middle = rest.astype(BF16)
    low = (rest - middle.astype(F32)).astype(BF16)
    return high, middle, low


def kernel(
    n_slab,
    n_tile,
    feat,
    counts,
    rb,
    face,
    w_one,
    gain_one,
    shift_one,
    w_two,
    gain_two,
    shift_two,
    out,
    weights,
    wt,
    face_hot,
    table,
    gathered,
    conv_out,
    send_face,
    halo,
    inbox,
    w_sem,
    halo_send,
    halo_recv,
    red_send,
    red_recv,
):
    s = lax.axis_index("slab")
    t = lax.axis_index("tile")
    rows = feat.shape[2]
    chans = feat.shape[3]
    up_s, down_s = lax.rem(s + 1, n_slab), lax.rem(s + n_slab - 1, n_slab)
    up_t, down_t = lax.rem(t + 1, n_tile), lax.rem(t + n_tile - 1, n_tile)
    sides = (
        (down_s, t),
        (up_s, t),
        (s, down_t),
        (s, up_t),
        (up_s, down_t),
        (up_s, up_t),
        (down_s, down_t),
        (down_s, up_t),
    )
    inner = lax.rem(s, RING)
    outer = s // RING

    def peer(phase, step):
        if phase == 0:
            return (s, lax.rem(t + step, RING))
        if phase == 1:
            return (outer * RING + lax.rem(inner + step, RING), t)
        return (lax.rem(outer + step, RING) * RING + inner, t)

    slot_of = (t, inner, outer)

    barrier = pltpu.get_barrier_semaphore()
    for device in sides:
        pl.semaphore_signal(barrier, inc=1, device_id=device, device_id_type=MESH)
    for phase in range(3):
        for step in range(1, RING):
            pl.semaphore_signal(
                barrier, inc=1, device_id=peer(phase, step), device_id_type=MESH
            )

    loads = [
        pltpu.make_async_copy(w, weights.at[i], w_sem.at[i])
        for i, w in enumerate((w_one, w_two))
    ]
    for load in loads:
        load.start()

    count = counts[0, 0]
    live = lax.broadcasted_iota(jnp.int32, (rows, chans), 0) < count
    features = feat[0, 0].astype(F32)

    row_id = lax.broadcasted_iota(jnp.int32, (rows, 64), 0)
    for j in range(4):
        hot = row_id == face[0, 0, j : j + 1, :]
        face_hot[:, j * 64 : (j + 1) * 64] = jnp.where(hot, 1.0, 0.0).astype(BF16)

    def start_exchange(e, source):
        parts = [p.astype(F32).T.astype(BF16) for p in thirds(source)]
        picked = jnp.dot(
            jnp.concatenate(parts, axis=0), face_hot[...], preferred_element_type=F32
        )
        total = picked[:chans] + picked[chans : 2 * chans] + picked[2 * chans :]
        send_face[e] = total.T
        moves = (
            (0, 64, 64),
            (64, 64, 0),
            (128, 64, 216),
            (192, 64, 136),
            (64, 8, 208),
            (120, 8, 128),
            (0, 8, 280),
            (56, 8, 200),
        )
        copies = []
        for i, (start, size, target) in enumerate(moves):
            copies.append(
                pltpu.make_async_remote_copy(
                    src_ref=send_face.at[e, pl.ds(start, size)],
                    dst_ref=halo.at[e, pl.ds(target, size)],
                    send_sem=halo_send.at[e, i],
                    recv_sem=halo_recv.at[e, i],
                    device_id=sides[i],
                    device_id_type=MESH,
                )
            )
        return copies

    has_down_s, has_up_s = s > 0, s < n_slab - 1
    has_down_t, has_up_t = t > 0, t < n_tile - 1

    def received(e, blank):
        pieces = (
            (0, 64, has_down_s),
            (64, 64, has_up_s),
            (128, 8, has_down_s & has_down_t),
            (136, 64, has_down_t),
            (200, 8, has_up_s & has_down_t),
            (208, 8, has_down_s & has_up_t),
            (216, 64, has_up_t),
            (280, 8, has_up_s & has_up_t),
        )
        return jnp.concatenate(
            [
                jnp.where(present, halo[e, pl.ds(start, size), :], blank)
                for start, size, present in pieces
            ],
            axis=0,
        )

    def convolve(c, local, around):
        pad = jnp.zeros((HALF + 64 - HALO, chans), F32)
        low = jnp.concatenate([around[:64], around[128:], pad], axis=0)
        high = jnp.concatenate([around[64:], pad], axis=0)
        for i in range(2):
            table[i, :chans] = local[:HALF].T.astype(BF16)
            table[i, chans : 2 * chans] = local[HALF:].T.astype(BF16)
        table[0, 2 * chans :] = low.T.astype(BF16)
        table[1, 2 * chans :] = high.T.astype(BF16)

        position = lax.broadcasted_iota(jnp.int32, (HALF, rows), 0)

        def tap(k, carry):
            index = rb[0, 0, pl.ds(k, 1), :]
            slot = jnp.where(
                index < 2 * HALF,
                index & (HALF - 1),
                jnp.where(index < 576, index - 512, index - 576),
            )
            hot = jnp.where(position == slot, 1.0, 0.0).astype(BF16)
            side = jnp.where(k < 9, 0, 1)
            found = jnp.dot(table[side], hot, preferred_element_type=F32)
            value = jnp.where(
                index < HALF,
                found[:chans],
                jnp.where(index < 2 * HALF, found[chans : 2 * chans], found[2 * chans :]),
            )
            gathered[pl.ds(pl.multiple_of(k * chans, chans), chans), :] = value.astype(BF16)
            return carry

        lax.fori_loop(0, TAPS, tap, 0)
        result = jnp.dot(wt[c], gathered[...], preferred_element_type=F32)
        conv_out[c] = result.T

    def transpose_weights(c):
        def one(k, carry):
            wt[c, :, pl.ds(pl.multiple_of(k * chans, chans), chans)] = weights[c, k].T
            return carry

        lax.fori_loop(0, TAPS, one, 0)

    copies = []

    def reduce_start(c, phase, value):
        slot = slot_of[phase]
        inbox[c, phase, slot] = value
        started = []
        for step in range(1, RING):
            copy = pltpu.make_async_remote_copy(
                src_ref=inbox.at[c, phase, slot],
                dst_ref=inbox.at[c, phase, slot],
                send_sem=red_send.at[c, phase, step],
                recv_sem=red_recv.at[c, phase, step],
                device_id=peer(phase, step),
                device_id_type=MESH,
            )
            copy.start()
            started.append(copy)
        copies.extend(started)
        return started

    def reduce_end(c, phase, started):
        for copy in started:
            copy.wait_recv()
        return jnp.sum(inbox[c, phase], axis=0)

    def message(c):
        value = jnp.where(live, conv_out[c], 0.0)
        sums = jnp.sum(value, axis=0, keepdims=True)
        squares = jnp.sum(value * value, axis=0, keepdims=True)
        row = lax.broadcasted_iota(jnp.int32, (4, chans), 0)
        counted = jnp.where(row == 2, count.astype(F32), 0.0)
        return jnp.where(row == 0, sums, jnp.where(row == 1, squares, counted))

    def moments(total):
        voxels = total[2:3]
        mean = total[0:1] / voxels
        variance = total[1:2] / voxels - mean * mean
        return mean, variance

    pl.semaphore_wait(barrier, 8 + 3 * (RING - 1))
    first_halo = start_exchange(0, features)
    for copy in first_halo:
        copy.start()
    loads[0].wait()
    transpose_weights(0)
    for copy in first_halo:
        copy.wait_recv()
    convolve(0, features, received(0, 0.0))

    started = reduce_start(0, 0, message(0))
    raw = jnp.where(live, conv_out[0], DEAD)
    second_halo = start_exchange(1, raw)
    for copy in second_halo:
        copy.start()
    loads[1].wait()
    transpose_weights(1)
    total = reduce_end(0, 0, started)
    started = reduce_start(0, 1, total)
    total = reduce_end(0, 1, started)
    started = reduce_start(0, 2, total)
    total = reduce_end(0, 2, started)
    mean, variance = moments(total)
    scale = lax.rsqrt(variance + EPSILON) * gain_one[...]

    def activate(x):
        return jnp.maximum((x - mean) * scale + shift_one[...], 0.0)

    for copy in second_halo:
        copy.wait_recv()
    hidden = jnp.where(live, activate(conv_out[0]), 0.0)
    convolve(1, hidden, activate(received(1, DEAD)))

    total = message(1)
    for phase in range(3):
        started = reduce_start(1, phase, total)
        total = reduce_end(1, phase, started)
    mean, variance = moments(total)
    scale = lax.rsqrt(variance + EPSILON) * gain_two[...]
    summed = (conv_out[1] - mean) * scale + shift_two[...] + feat[0, 0].astype(F32)
    out[0, 0] = jnp.where(live, jnp.maximum(summed, 0.0), 0.0).astype(BF16)

    for copy in first_halo + second_halo + copies:
        copy.wait_send()


def solution(mesh):
    n_slab, n_tile = mesh.shape["slab"], mesh.shape["tile"]

    def per_device(
        features,
        counts,
        rulebook,
        face_rows,
        conv_one,
        gain_one,
        shift_one,
        conv_two,
        gain_two,
        shift_two,
    ):
        rows, chans = features.shape[2], features.shape[3]
        vmem = pl.BlockSpec(memory_space=pltpu.VMEM)
        hbm = pl.BlockSpec(memory_space=pl.ANY)
        smem = pl.BlockSpec(memory_space=pltpu.SMEM)
        line = (1, chans)
        return pl.pallas_call(
            functools.partial(kernel, n_slab, n_tile),
            out_shape=jax.ShapeDtypeStruct(features.shape, features.dtype),
            in_specs=[vmem, smem, vmem, vmem, hbm, vmem, vmem, hbm, vmem, vmem],
            out_specs=vmem,
            scratch_shapes=[
                pltpu.VMEM((2, TAPS, chans, chans), BF16),
                pltpu.VMEM((2, chans, TAPS * chans), BF16),
                pltpu.VMEM((rows, 256), BF16),
                pltpu.VMEM((2, 3 * chans, HALF), BF16),
                pltpu.VMEM((TAPS * chans, rows), BF16),
                pltpu.VMEM((2, rows, chans), F32),
                pltpu.VMEM((2, 256, chans), F32),
                pltpu.VMEM((2, HALO, chans), F32),
                pltpu.VMEM((2, 3, RING, 4, chans), F32),
                pltpu.SemaphoreType.DMA((2,)),
                pltpu.SemaphoreType.DMA((2, 8)),
                pltpu.SemaphoreType.DMA((2, 8)),
                pltpu.SemaphoreType.DMA((2, 3, RING)),
                pltpu.SemaphoreType.DMA((2, 3, RING)),
            ],
            compiler_params=pltpu.CompilerParams(
                collective_id=0,
                has_side_effects=True,
                vmem_limit_bytes=60 * 1024 * 1024,
            ),
        )(
            features,
            counts,
            rulebook,
            face_rows,
            conv_one,
            gain_one.reshape(line),
            shift_one.reshape(line),
            conv_two,
            gain_two.reshape(line),
            shift_two.reshape(line),
        )

    grid = P("slab", "tile", None, None)
    return jax.shard_map(
        per_device,
        mesh=mesh,
        in_specs=(grid, P("slab", "tile"), grid, grid, P(), P(), P(), P(), P(), P()),
        out_specs=grid,
        check_vma=False,
    )
```
